32 devices in a mesh: row: 4 (over y, x), col: 8 (over z, core).
Axes of the slice: x: 2, y: 2, z: 4, core: 2. Of those that a mesh axis runs over, the one named last changes fastest.
Arguments:
- object_field: float32 [2, 1024, 2048], P(None, 'row', 'col'), may hold values from -6 to 6
- probe_modes: float32 [4, 2, 256, 256], replicated, may hold values from -3 to 3
- positions: int32 [4, 8, 6, 2], P('row', 'col'), may hold values from 0 to 255
- counts: int32 [4, 8], P('row', 'col'), may hold values from 0 to 6, as said below
- amplitude: float32 [4, 8, 6, 256, 256], P('row', 'col'), may hold values from 0 to 2
Outputs:
- updated: float32 [2, 1024, 2048], P(None, 'row', 'col')
The draws below stay inside these ranges and needn't reach their ends.
Inputs may be any that keep to these rules, and one draw needn't show every extreme that they name: The counts of two tiles in one tile row whose column indices differ by 4 add up to 6; some tile has exactly 6. Only positions below a tile's count are used.
All inputs are finite; a program needn't handle non-finite values.
Results may differ from the reference program's by a relative error of at most 0.0018.
Values sent between devices are 32-bit elements; how exact they have to be, the bound alone decides.
A program may use at most 64 MiB of HBM per device.

```python
import math
import jax
import jax.numpy as jnp
from jax import lax

PATCH = 256
MODES = 4
TILE = 256
SLOTS = 3
ITERS = 2
SURPLUS = 3
MOST = 6
TILES_R = 4
TILES_C = 8
ROWS = 1024
COLS = 2048


def draw_counts(key, part):
    half = TILES_C // 2
    first = jax.random.fold_in(key, 11)
    second = jax.random.fold_in(key, 23)
    base = jax.random.randint(first, (TILES_R, half), SLOTS - SURPLUS, SLOTS + SURPLUS + 1)
    spot = jax.random.randint(second, (), 0, TILES_R * half)
    flat = jnp.where(jnp.arange(TILES_R * half) == spot, MOST, base.reshape(-1))
    base = flat.reshape(TILES_R, half)
    return jnp.concatenate([base, 2 * SLOTS - base], axis=1).astype(jnp.int32)


def set_ends(result, own_key, least, top_value):
    longest = result.shape.index(max(result.shape))
    spots = []
    for shift in (0, 1):
        where = [jax.random.randint(jax.random.fold_in(own_key, axis), (), 0, length) for axis, length in enumerate(result.shape)]
        where[longest] = (where[longest] + shift) % result.shape[longest]
        spots.append(tuple(where))
    return result.at[spots[0]].set(least).at[spots[1]].set(top_value)


def shard_levels(key, dims, split, least, largest):
    def one(dim, shards_of):
        heights = jax.random.uniform(jax.random.fold_in(jax.random.fold_in(key, 6), dim), (shards_of,), jnp.float32, least / len(split), largest / len(split))
        return jnp.repeat(jnp.exp(heights), dims[dim] // shards_of).reshape((-1,) + (1,) * (len(dims) - dim - 1))

    gain = one(*split[0])
    for cut in split[1:]:
        gain = gain * one(*cut)
    return gain


def scatter_about(key, extent, deviation, most, shards=(), held_as=jnp.bfloat16):
    entries = jax.random.normal(key, extent, jnp.float32) * deviation
    if len(shards) > 0:
        entries = shard_levels(key, extent, shards, -0.22, 0.18) * entries
    return jnp.clip(entries, min=-most, max=most).astype(held_as)


def setup_inputs(seed: int = 0) -> dict:
    splits = jax.random.split(jax.random.key(seed), 6)
    return {
        "object_field": scatter_about(splits[0], (2, ROWS, COLS), 1.0, 6.0, ((1, 4), (2, 8)), jnp.float32),
        "probe_modes": scatter_about(splits[1], (MODES, 2, PATCH, PATCH), 0.5, 3.0, (), jnp.float32),
        "positions": set_ends(jax.random.randint(splits[2], (TILES_R, TILES_C, MOST, 2), 0, TILE), jax.random.fold_in(splits[2], 1), 0, TILE - 1).astype(jnp.int32),
        "counts": draw_counts(jax.random.fold_in(splits[5], 71), 0),
        "amplitude": jnp.clip(2.0 * jax.random.uniform(splits[4], (TILES_R, TILES_C, MOST, PATCH, PATCH), jnp.float32) ** shard_levels(splits[4], (TILES_R, TILES_C, MOST, PATCH, PATCH), ((0, 4), (1, 8)), -0.2, 0.2), 0.0, 2.0),
    }


step_size = 0.1
damping = 0.1

def blocks(upper_left, upper_right, lower_left, lower_right):
    return jnp.stack([jnp.stack([upper_left, upper_right], axis=1), jnp.stack([lower_left, lower_right], axis=1)], axis=0)

def tables():
    ladder = jnp.arange(PATCH, dtype=jnp.int32)
    product = ladder[:, None] * ladder[None, :] % PATCH
    theta = product.astype(jnp.float32) * (2.0 * math.pi / PATCH)
    factor = 1.0 / math.sqrt(PATCH)
    cosine = jnp.cos(theta) * factor
    minus_sine = -jnp.sin(theta) * factor
    table_fwd = blocks(cosine, -minus_sine, minus_sine, cosine).astype(jnp.bfloat16)
    table_inv = blocks(cosine, minus_sine, -minus_sine, cosine).astype(jnp.bfloat16)
    return (table_fwd, table_inv)

def left_mult(table, values):
    return jnp.einsum('cjdk,mdkl->mcjl', table.astype(jnp.float32), values.astype(jnp.float32), precision=lax.Precision.HIGHEST)

def right_mult(values, table):
    return jnp.einsum('mcjk,ckdl->mdjl', values.astype(jnp.float32), table.astype(jnp.float32), precision=lax.Precision.HIGHEST)

def patch_gradient(patch, measured, probe_modes, table_fwd, table_inv):
    probe_re = probe_modes[:, 0]
    probe_im = probe_modes[:, 1]
    psi = jnp.stack([probe_re * patch[0] - probe_im * patch[1], probe_re * patch[1] + probe_im * patch[0]], axis=1).astype(jnp.bfloat16)
    section = left_mult(table_fwd, psi).astype(jnp.bfloat16)
    far = right_mult(section, table_inv)
    intensity = lax.optimization_barrier(jnp.sum(far * far, axis=(0, 1)))
    ratio = 1.0 - measured / jnp.sqrt(intensity + damping)
    chi = (far * ratio).astype(jnp.bfloat16)
    back = left_mult(table_inv, chi).astype(jnp.bfloat16)
    wave = right_mult(back, table_fwd)
    grad_re = lax.optimization_barrier(jnp.sum(probe_re * wave[:, 0] + probe_im * wave[:, 1], axis=0))
    grad_im = lax.optimization_barrier(jnp.sum(probe_re * wave[:, 1] - probe_im * wave[:, 0], axis=0))
    return jnp.stack([grad_re, grad_im], axis=0)

def reference(object_field, probe_modes, positions, counts, amplitude):
    table_fwd, table_inv = tables()
    tile_rows, tile_cols = counts.shape
    slot_ids = jnp.arange(MOST, dtype=jnp.int32)
    live = (slot_ids[None, None, :] < counts[:, :, None]).reshape(-1)
    order = jnp.argsort(jnp.where(live, 0, 1).astype(jnp.int32), stable=True)[:SLOTS * tile_rows * tile_cols].astype(jnp.int32)
    tile_row = order // (tile_cols * MOST)
    tile_col = order // MOST % tile_cols
    offsets = positions.reshape(-1, 2)
    top_rows = (tile_row * TILE + offsets[order, 0]).astype(jnp.int32)
    left_cols = (tile_col * TILE + offsets[order, 1]).astype(jnp.int32)
    measured_all = amplitude.reshape(-1, PATCH, PATCH)
    anchor = jnp.int32(0)
    field = object_field
    for sweep in range(ITERS):
        padded = jnp.pad(field, ((0, 0), (0, PATCH), (0, PATCH)))

        def visit(total, entry):
            which, top, left = entry
            patch = lax.dynamic_slice(padded, (anchor, top, left), (2, PATCH, PATCH))
            measured = lax.dynamic_index_in_dim(measured_all, which, 0, keepdims=False)
            grads = patch_gradient(patch, measured, probe_modes, table_fwd, table_inv)
            current = lax.dynamic_slice(total, (anchor, top, left), (2, PATCH, PATCH))
            return (lax.dynamic_update_slice(total, current + grads, (anchor, top, left)), None)
        total, unused = lax.scan(visit, jnp.zeros_like(padded), (order, top_rows, left_cols))
        field = field - step_size * total[:, :ROWS, :COLS]
    return field
```

```python
import math

import jax
import jax.numpy as jnp
import numpy as np
from jax import lax
from jax.experimental import pallas as pl
from jax.experimental.pallas import tpu as pltpu
from jax.sharding import PartitionSpec as P

ITERS = 2


step_size = 0.1
damping = 0.1


def from_behind(block, axis, distance):
    devices = range(lax.axis_size(axis))
    route = [(i - distance, i) for i in devices if i - distance in devices]
    return lax.ppermute(block, axis, route)


def tables(width):
    half = width // 2
    ladder = np.arange(width)
    theta = (ladder[:, None] * ladder[None, :] % width) * (2.0 * math.pi / width)
    factor = 1.0 / math.sqrt(width)
    cosine = np.cos(theta) * factor
    sine = np.sin(theta) * factor
    out = []
    for parity in (0, 1):
        c = cosine[parity::2, :half]
        s = sine[parity::2, :half]
        out.append(np.block([[c, s], [-s, c]]))
    stacked = np.stack(out).astype(np.float32)
    fwd = jnp.asarray(stacked).astype(jnp.bfloat16)
    inv = jnp.asarray(np.ascontiguousarray(stacked.transpose(0, 2, 1))).astype(jnp.bfloat16)
    return fwd, inv


def dot(a, b):
    return jnp.dot(a, b, preferred_element_type=jnp.float32)


def gradient_kernel(
    count_ref,
    pos_ref,
    ext_ref,
    amp_ref,
    probe_ref,
    a_ref,
    b_ref,
    tot_ref,
    patch_scr,
    psi_scr,
    x_scr,
    far_scr,
    chi_scr,
    y_scr,
    grad_scr,
):
    modes, _, width, _ = probe_ref.shape
    h = width // 2
    lane = 128
    wide = width + lane
    tot_ref[...] = jnp.zeros_like(tot_ref)
    sub = 8
    blocks = width // sub
    step = 16

    def slot(s, carry):
        top = pos_ref[0, 0, s, 0]
        left = pos_ref[0, 0, s, 1]
        base = pl.multiple_of((left // lane) * lane, lane)
        rest = left - base
        over = pl.multiple_of((top // sub) * sub, sub)
        drop = top - over
        lanes = lax.broadcasted_iota(jnp.int32, (width, lane), 1)
        ledge = lax.broadcasted_iota(jnp.int32, (blocks, sub, lane), 1)
        for d in range(2):
            turned = []
            for c in range(wide // lane):
                cols = pl.ds(pl.multiple_of(base + c * lane, lane), lane)
                x = ext_ref[d, pl.ds(over, width + sub), cols].reshape(blocks + 1, sub, lane)
                x = pltpu.roll(x, lax.rem(sub - drop, sub), 1)
                x = jnp.where(ledge + drop < sub, x[:-1], x[1:]).reshape(width, lane)
                turned.append(pltpu.roll(x, lax.rem(lane - rest, lane), 1))
            for c in range(width // lane):
                patch_scr[d, :, c * lane : (c + 1) * lane] = jnp.where(
                    lanes + rest < lane, turned[c], turned[c + 1]
                )
        for m in range(modes):
            for r in range(0, h, step):
                rows = slice(r, r + step)
                low = slice(h + r, h + r + step)
                pr, pi = probe_ref[m, 0, rows], probe_ref[m, 1, rows]
                qr, qi = probe_ref[m, 0, low], probe_ref[m, 1, low]
                fr, fi = patch_scr[0, rows], patch_scr[1, rows]
                gr, gi = patch_scr[0, low], patch_scr[1, low]
                ur, ui = pr * fr - pi * fi, pr * fi + pi * fr
                vr, vi = qr * gr - qi * gi, qr * gi + qi * gr
                psi_scr[m, 0, rows] = (ur + vr).astype(jnp.bfloat16)
                psi_scr[m, 0, low] = (ui + vi).astype(jnp.bfloat16)
                psi_scr[m, 1, rows] = (ur - vr).astype(jnp.bfloat16)
                psi_scr[m, 1, low] = (ui - vi).astype(jnp.bfloat16)
            for p in range(2):
                out = dot(a_ref[p], psi_scr[m, p])
                re_l, re_r = out[:h, :h], out[:h, h:]
                im_l, im_r = out[h:, :h], out[h:, h:]
                rows = slice(p * h, (p + 1) * h)
                x_scr[m, 0, rows, :h] = (re_l + re_r).astype(jnp.bfloat16)
                x_scr[m, 0, rows, h:] = (im_l + im_r).astype(jnp.bfloat16)
                x_scr[m, 1, rows, :h] = (re_l - re_r).astype(jnp.bfloat16)
                x_scr[m, 1, rows, h:] = (im_l - im_r).astype(jnp.bfloat16)
            for q in range(2):
                far_scr[m, q] = dot(x_scr[m, q], b_ref[q])
        for p in range(2):
            for q in range(2):
                cols = slice(q * h, (q + 1) * h)
                for r in range(0, h, step):
                    rows = slice(p * h + r, p * h + r + step)
                    total = None
                    for m in range(modes):
                        re, im = far_scr[m, q, rows, :h], far_scr[m, q, rows, h:]
                        term = re * re + im * im
                        total = term if total is None else total + term
                    ratio = 1.0 - amp_ref[s, rows, cols] * lax.rsqrt(total + damping)
                    for m in range(modes):
                        re, im = far_scr[m, q, rows, :h], far_scr[m, q, rows, h:]
                        chi_scr[m, p, r : r + step, cols] = (re * ratio).astype(jnp.bfloat16)
                        chi_scr[m, p, h + r : h + r + step, cols] = (im * ratio).astype(
                            jnp.bfloat16
                        )
        for m in range(modes):
            even = dot(b_ref[0], chi_scr[m, 0])
            odd = dot(b_ref[1], chi_scr[m, 1])
            upper = (even + odd).astype(jnp.bfloat16)
            lower = (even - odd).astype(jnp.bfloat16)
            for q in range(2):
                cols = slice(q * h, (q + 1) * h)
                y_scr[m, q, :h, :h] = upper[:h, cols]
                y_scr[m, q, :h, h:] = upper[h:, cols]
                y_scr[m, q, h:, :h] = lower[:h, cols]
                y_scr[m, q, h:, h:] = lower[h:, cols]
            even = dot(y_scr[m, 0], a_ref[0])
            odd = dot(y_scr[m, 1], a_ref[1])
            for cols, wave in ((slice(0, h), even + odd), (slice(h, width), even - odd)):
                wr, wi = wave[:, :h], wave[:, h:]
                pr, pi = probe_ref[m, 0, :, cols], probe_ref[m, 1, :, cols]
                gr, gi = pr * wr + pi * wi, pr * wi - pi * wr
                if m > 0:
                    gr, gi = grad_scr[0, :, cols] + gr, grad_scr[1, :, cols] + gi
                grad_scr[0, :, cols] = gr
                grad_scr[1, :, cols] = gi
        for d in range(2):
            edge = jnp.zeros((width, lane), jnp.float32)
            turned = [edge]
            for c in range(width // lane):
                x = grad_scr[d, :, c * lane : (c + 1) * lane]
                turned.append(pltpu.roll(x, rest, 1))
            turned.append(edge)
            for c in range(wide // lane):
                x = jnp.where(lanes >= rest, turned[c + 1], turned[c])
                x = pltpu.roll(x.reshape(blocks, sub, lane), drop, 1)
                brim = jnp.zeros((1, sub, lane), jnp.float32)
                after = jnp.concatenate([x, brim], axis=0)
                before = jnp.concatenate([brim, x], axis=0)
                rim = lax.broadcasted_iota(jnp.int32, (blocks + 1, sub, lane), 1)
                x = jnp.where(rim >= drop, after, before).reshape(width + sub, lane)
                cols = pl.ds(pl.multiple_of(base + c * lane, lane), lane)
                spot = (d, pl.ds(over, width + sub), cols)
                tot_ref[spot] = tot_ref[spot] + x
        return carry

    lax.fori_loop(0, count_ref[0, 0], slot, 0)


def gradient(counts, positions, extended, amp, probe_modes, fwd, inv):
    modes, _, width, _ = probe_modes.shape
    vmem = pl.BlockSpec(memory_space=pltpu.VMEM)
    smem = pl.BlockSpec(memory_space=pltpu.SMEM)
    return pl.pallas_call(
        gradient_kernel,
        out_shape=jax.ShapeDtypeStruct(extended.shape, jnp.float32),
        in_specs=[smem, smem] + [vmem] * 5,
        out_specs=vmem,
        scratch_shapes=[
            pltpu.VMEM((2, width, width), jnp.float32),
            pltpu.VMEM((modes, 2, width, width), jnp.bfloat16),
            pltpu.VMEM((modes, 2, width, width), jnp.bfloat16),
            pltpu.VMEM((modes, 2, width, width), jnp.float32),
            pltpu.VMEM((modes, 2, width, width), jnp.bfloat16),
            pltpu.VMEM((modes, 2, width, width), jnp.bfloat16),
            pltpu.VMEM((2, width, width), jnp.float32),
        ],
        compiler_params=pltpu.CompilerParams(vmem_limit_bytes=40 * 1024 * 1024),
        name="gradient",
    )(counts, positions, extended, amp, probe_modes, fwd, inv)


def exact(values, product):
    total = None
    for _ in range(3):
        piece = values.astype(jnp.bfloat16)
        values = values - piece.astype(jnp.float32)
        part = product(piece)
        total = part if total is None else total + part
    return total


def sort_kernel(amp_ref, perm_ref, back_ref, out_ref):
    def one(s, carry):
        cols = exact(amp_ref[s], lambda piece: dot(piece, perm_ref[...]))
        out_ref[s] = exact(cols, lambda piece: dot(back_ref[...], piece))
        return carry

    lax.fori_loop(0, amp_ref.shape[0], one, 0)


def sort_amplitude(amp):
    width = amp.shape[-1]
    perm = np.zeros((width, width), np.float32)
    order = np.concatenate([np.arange(0, width, 2), np.arange(1, width, 2)])
    perm[order, np.arange(width)] = 1.0
    return pl.pallas_call(
        sort_kernel,
        out_shape=jax.ShapeDtypeStruct(amp.shape, jnp.float32),
        in_specs=[pl.BlockSpec(memory_space=pltpu.VMEM)] * 3,
        out_specs=pl.BlockSpec(memory_space=pltpu.VMEM),
        cost_estimate=pl.CostEstimate(
            flops=12 * width**3 * amp.shape[0],
            bytes_accessed=8 * amp.size,
            transcendentals=0,
        ),
        name="sort_amplitude",
    )(amp, jnp.asarray(perm).astype(jnp.bfloat16), jnp.asarray(perm.T).astype(jnp.bfloat16))


def body(object_field, probe_modes, positions, counts, amplitude):
    width = probe_modes.shape[-1]
    tile = object_field.shape[1]
    fwd, inv = tables(width)
    amp = sort_amplitude(amplitude[0, 0])
    field = object_field
    for sweep in range(ITERS):
        below = from_behind(field, "row", -1)
        column = jnp.concatenate([field, below], axis=1)
        beside = from_behind(column, "col", -1)
        extended = jnp.concatenate([column, beside], axis=2)
        total = gradient(counts, positions, extended, amp, probe_modes, fwd, inv)
        from_left = from_behind(total[:, :, tile:], "col", 1)
        column_sum = total[:, :, :tile] + from_left
        from_above = from_behind(column_sum[:, tile:], "row", 1)
        field = field - step_size * (column_sum[:, :tile] + from_above)
    return field


def solution(mesh):
    placed = (
        P(None, "row", "col"),
        P(),
        P("row", "col", None, None),
        P("row", "col"),
        P("row", "col", None, None, None),
    )
    return jax.shard_map(
        body, mesh=mesh, in_specs=placed, out_specs=P(None, "row", "col"), check_vma=False
    )
```

```python
import functools
import math

import jax
import jax.numpy as jnp
import numpy as np
from jax import lax
from jax.experimental import pallas as pl
from jax.experimental.pallas import tpu as pltpu
from jax.sharding import PartitionSpec as P

ITERS = 2


step_size = 0.1
damping = 0.1


RIGHT_LOW, RIGHT_TOP, DOWN, UP, LEFT, PASS_ON = range(6)
PARTS = 4


def exchange_kernel(reduce, spread, rows_of, cols_of, *refs):
    refs = list(refs)
    tot_ref = refs.pop(0) if reduce else None
    field_ref = refs.pop(0)
    new_ref = refs.pop(0) if reduce else field_ref
    ext_ref = refs.pop(0) if spread else None
    if reduce:
        side_scr, low_scr, above_scr = refs.pop(0), refs.pop(0), refs.pop(0)
    send_sem, recv_sem = refs
    t = field_ref.shape[1]
    chunk = t // PARTS
    r, c = lax.axis_index("row"), lax.axis_index("col")
    has_up, has_down = r > 0, r < rows_of - 1
    has_left, has_right = c > 0, c < cols_of - 1
    up = (jnp.where(has_up, r - 1, r + 1), c)
    down = (jnp.where(has_down, r + 1, r - 1), c)
    left = (r, jnp.where(has_left, c - 1, c + 1))
    right = (r, jnp.where(has_right, c + 1, c - 1))

    barrier = pltpu.get_barrier_semaphore()
    for there, device in ((has_up, up), (has_down, down), (has_left, left), (has_right, right)):

        @pl.when(there)
        def _():
            pl.semaphore_signal(
                barrier, inc=1, device_id=device, device_id_type=pl.DeviceIdType.MESH
            )

    peers = sum(jnp.where(there, 1, 0) for there in (has_up, has_down, has_left, has_right))
    pl.semaphore_wait(barrier, peers)

    def copy(kind, i):
        rows = pl.ds(i * chunk, chunk)
        low = pl.ds(t + i * chunk, chunk)
        near, far = pl.ds(0, t), pl.ds(t, t)
        if kind == RIGHT_LOW:
            src, dst, device = tot_ref.at[:, low, far], side_scr.at[:, low, :], right
        elif kind == RIGHT_TOP:
            src, dst, device = tot_ref.at[:, rows, far], side_scr.at[:, rows, :], right
        elif kind == DOWN:
            src, dst, device = low_scr.at[:, rows, :], above_scr.at[:, rows, :], down
        elif kind == UP:
            src, dst, device = new_ref.at[:, rows, :], ext_ref.at[:, low, near], up
        elif kind == LEFT:
            src, dst, device = new_ref.at[:, rows, :], ext_ref.at[:, rows, far], left
        else:
            src, dst, device = ext_ref.at[:, low, near], ext_ref.at[:, low, far], left
        return pltpu.make_async_remote_copy(
            src_ref=src,
            dst_ref=dst,
            send_sem=send_sem.at[kind, i],
            recv_sem=recv_sem.at[kind, i],
            device_id=device,
            device_id_type=pl.DeviceIdType.MESH,
        )

    def start(there, kind, i):
        @pl.when(there)
        def _():
            copy(kind, i).start()

    def got(there, kind, i):
        @pl.when(there)
        def _():
            copy(kind, i).wait_recv()

    def sent(there, kind):
        @pl.when(there)
        def _():
            for i in range(PARTS):
                copy(kind, i).wait_send()

    def pass_on(i):
        got(has_down, UP, i)
        start(jnp.logical_and(has_down, has_left), PASS_ON, i)

    if reduce:
        for kind in (RIGHT_LOW, RIGHT_TOP):
            for i in range(PARTS):
                start(has_right, kind, i)

        @pl.when(jnp.logical_not(has_left))
        def _():
            side_scr[...] = jnp.zeros_like(side_scr)

        @pl.when(jnp.logical_not(has_up))
        def _():
            above_scr[...] = jnp.zeros_like(above_scr)

    if spread:

        @pl.when(jnp.logical_not(has_down))
        def _():
            ext_ref[:, t:, :] = jnp.zeros((2, t, 2 * t), jnp.float32)

        @pl.when(jnp.logical_not(has_right))
        def _():
            ext_ref[:, :, t:] = jnp.zeros((2, 2 * t, t), jnp.float32)

    if reduce:
        for i in range(PARTS):
            rows = slice(i * chunk, (i + 1) * chunk)
            low = slice(t + i * chunk, t + (i + 1) * chunk)
            got(has_left, RIGHT_LOW, i)

            @pl.when(has_down)
            def _():
                low_scr[:, rows, :] = tot_ref[:, low, :t] + side_scr[:, low, :]
                copy(DOWN, i).start()

    lag = 2
    for i in range(PARTS):
        rows = slice(i * chunk, (i + 1) * chunk)
        if reduce:
            got(has_left, RIGHT_TOP, i)
            got(has_up, DOWN, i)
            new_ref[:, rows, :] = field_ref[:, rows, :] - step_size * (
                tot_ref[:, rows, :t] + side_scr[:, rows, :] + above_scr[:, rows, :]
            )
        if spread:
            start(has_up, UP, i)
            start(has_left, LEFT, i)
            ext_ref[:, rows, :t] = new_ref[:, rows, :]
            if reduce and i >= lag:
                pass_on(i - lag)
    if spread:
        for i in range(PARTS - lag if reduce else 0, PARTS):
            pass_on(i)
        for i in range(PARTS):
            got(has_right, LEFT, i)
            got(jnp.logical_and(has_right, has_down), PASS_ON, i)
    if reduce:
        sent(has_right, RIGHT_LOW)
        sent(has_right, RIGHT_TOP)
        sent(has_down, DOWN)
    if spread:
        sent(has_up, UP)
        sent(has_left, LEFT)
        sent(jnp.logical_and(has_down, has_left), PASS_ON)


def exchange(total, field, spread):
    reduce = total is not None
    planes, t, _ = field.shape
    vmem = pl.BlockSpec(memory_space=pltpu.VMEM)
    tile = jax.ShapeDtypeStruct(field.shape, jnp.float32)
    shapes = [tile] * reduce + [jax.ShapeDtypeStruct((planes, 2 * t, 2 * t), jnp.float32)] * spread
    scratch = []
    if reduce:
        scratch = [
            pltpu.VMEM((planes, 2 * t, t), jnp.float32),
            pltpu.VMEM((planes, t, t), jnp.float32),
            pltpu.VMEM((planes, t, t), jnp.float32),
        ]
    scratch += [pltpu.SemaphoreType.DMA((6, PARTS))] * 2
    kernel = functools.partial(
        exchange_kernel, reduce, spread, lax.axis_size("row"), lax.axis_size("col")
    )
    return pl.pallas_call(
        kernel,
        out_shape=shapes,
        in_specs=[vmem] * (1 + reduce),
        out_specs=[vmem] * len(shapes),
        scratch_shapes=scratch,
        compiler_params=pltpu.CompilerParams(
            collective_id=2 * reduce + spread,
            has_side_effects=True,
            vmem_limit_bytes=24 * 1024 * 1024,
        ),
        name="exchange",
    )(*([total] * reduce), field)


def tables(width):
    half = width // 2
    ladder = np.arange(width)
    theta = (ladder[:, None] * ladder[None, :] % width) * (2.0 * math.pi / width)
    factor = 1.0 / math.sqrt(width)
    cosine = np.cos(theta) * factor
    sine = np.sin(theta) * factor
    out = []
    for parity in (0, 1):
        c = cosine[parity::2, :half]
        s = sine[parity::2, :half]
        out.append(np.block([[c, s], [-s, c]]))
    stacked = np.stack(out).astype(np.float32)
    fwd = jnp.asarray(stacked).astype(jnp.bfloat16)
    inv = jnp.asarray(np.ascontiguousarray(stacked.transpose(0, 2, 1))).astype(jnp.bfloat16)
    return fwd, inv


def dot(a, b):
    return jnp.dot(a, b, preferred_element_type=jnp.float32)


def gradient_kernel(
    count_ref,
    pos_ref,
    ext_ref,
    amp_ref,
    probe_ref,
    a_ref,
    b_ref,
    tot_ref,
    patch_scr,
    psi_scr,
    x_scr,
    far_scr,
    chi_scr,
    y_scr,
    grad_scr,
):
    modes, _, width, _ = probe_ref.shape
    h = width // 2
    lane = 128
    wide = width + lane
    tot_ref[...] = jnp.zeros_like(tot_ref)
    sub = 8
    blocks = width // sub
    step = 16

    def slot(s, carry):
        top = pos_ref[0, 0, s, 0]
        left = pos_ref[0, 0, s, 1]
        base = pl.multiple_of((left // lane) * lane, lane)
        rest = left - base
        over = pl.multiple_of((top // sub) * sub, sub)
        drop = top - over
        lanes = lax.broadcasted_iota(jnp.int32, (width, lane), 1)
        ledge = lax.broadcasted_iota(jnp.int32, (blocks, sub, lane), 1)
        for d in range(2):
            turned = []
            for c in range(wide // lane):
                cols = pl.ds(pl.multiple_of(base + c * lane, lane), lane)
                x = ext_ref[d, pl.ds(over, width + sub), cols].reshape(blocks + 1, sub, lane)
                x = pltpu.roll(x, lax.rem(sub - drop, sub), 1)
                x = jnp.where(ledge + drop < sub, x[:-1], x[1:]).reshape(width, lane)
                turned.append(pltpu.roll(x, lax.rem(lane - rest, lane), 1))
            for c in range(width // lane):
                patch_scr[d, :, c * lane : (c + 1) * lane] = jnp.where(
                    lanes + rest < lane, turned[c], turned[c + 1]
                )
        for m in range(modes):
            for r in range(0, h, step):
                rows = slice(r, r + step)
                low = slice(h + r, h + r + step)
                pr, pi = probe_ref[m, 0, rows], probe_ref[m, 1, rows]
                qr, qi = probe_ref[m, 0, low], probe_ref[m, 1, low]
                fr, fi = patch_scr[0, rows], patch_scr[1, rows]
                gr, gi = patch_scr[0, low], patch_scr[1, low]
                ur, ui = pr * fr - pi * fi, pr * fi + pi * fr
                vr, vi = qr * gr - qi * gi, qr * gi + qi * gr
                psi_scr[m, 0, rows] = (ur + vr).astype(jnp.bfloat16)
                psi_scr[m, 0, low] = (ui + vi).astype(jnp.bfloat16)
                psi_scr[m, 1, rows] = (ur - vr).astype(jnp.bfloat16)
                psi_scr[m, 1, low] = (ui - vi).astype(jnp.bfloat16)
            for p in range(2):
                out = dot(a_ref[p], psi_scr[m, p])
                re_l, re_r = out[:h, :h], out[:h, h:]
                im_l, im_r = out[h:, :h], out[h:, h:]
                rows = slice(p * h, (p + 1) * h)
                x_scr[m, 0, rows, :h] = (re_l + re_r).astype(jnp.bfloat16)
                x_scr[m, 0, rows, h:] = (im_l + im_r).astype(jnp.bfloat16)
                x_scr[m, 1, rows, :h] = (re_l - re_r).astype(jnp.bfloat16)
                x_scr[m, 1, rows, h:] = (im_l - im_r).astype(jnp.bfloat16)
            for q in range(2):
                far_scr[m, q] = dot(x_scr[m, q], b_ref[q])
        for p in range(2):
            for q in range(2):
                cols = slice(q * h, (q + 1) * h)
                for r in range(0, h, step):
                    rows = slice(p * h + r, p * h + r + step)
                    total = None
                    for m in range(modes):
                        re, im = far_scr[m, q, rows, :h], far_scr[m, q, rows, h:]
                        term = re * re + im * im
                        total = term if total is None else total + term
                    ratio = 1.0 - amp_ref[s, rows, cols] * lax.rsqrt(total + damping)
                    for m in range(modes):
                        re, im = far_scr[m, q, rows, :h], far_scr[m, q, rows, h:]
                        chi_scr[m, p, r : r + step, cols] = (re * ratio).astype(jnp.bfloat16)
                        chi_scr[m, p, h + r : h + r + step, cols] = (im * ratio).astype(
                            jnp.bfloat16
                        )
        for m in range(modes):
            even = dot(b_ref[0], chi_scr[m, 0])
            odd = dot(b_ref[1], chi_scr[m, 1])
            upper = (even + odd).astype(jnp.bfloat16)
            lower = (even - odd).astype(jnp.bfloat16)
            for q in range(2):
                cols = slice(q * h, (q + 1) * h)
                y_scr[m, q, :h, :h] = upper[:h, cols]
                y_scr[m, q, :h, h:] = upper[h:, cols]
                y_scr[m, q, h:, :h] = lower[:h, cols]
                y_scr[m, q, h:, h:] = lower[h:, cols]
            even = dot(y_scr[m, 0], a_ref[0])
            odd = dot(y_scr[m, 1], a_ref[1])
            for cols, wave in ((slice(0, h), even + odd), (slice(h, width), even - odd)):
                wr, wi = wave[:, :h], wave[:, h:]
                pr, pi = probe_ref[m, 0, :, cols], probe_ref[m, 1, :, cols]
                gr, gi = pr * wr + pi * wi, pr * wi - pi * wr
                if m > 0:
                    gr, gi = grad_scr[0, :, cols] + gr, grad_scr[1, :, cols] + gi
                grad_scr[0, :, cols] = gr
                grad_scr[1, :, cols] = gi
        for d in range(2):
            edge = jnp.zeros((width, lane), jnp.float32)
            turned = [edge]
            for c in range(width // lane):
                x = grad_scr[d, :, c * lane : (c + 1) * lane]
                turned.append(pltpu.roll(x, rest, 1))
            turned.append(edge)
            for c in range(wide // lane):
                x = jnp.where(lanes >= rest, turned[c + 1], turned[c])
                x = pltpu.roll(x.reshape(blocks, sub, lane), drop, 1)
                brim = jnp.zeros((1, sub, lane), jnp.float32)
                after = jnp.concatenate([x, brim], axis=0)
                before = jnp.concatenate([brim, x], axis=0)
                rim = lax.broadcasted_iota(jnp.int32, (blocks + 1, sub, lane), 1)
                x = jnp.where(rim >= drop, after, before).reshape(width + sub, lane)
                cols = pl.ds(pl.multiple_of(base + c * lane, lane), lane)
                spot = (d, pl.ds(over, width + sub), cols)
                tot_ref[spot] = tot_ref[spot] + x
        return carry

    lax.fori_loop(0, count_ref[0, 0], slot, 0)


def gradient(counts, positions, extended, amp, probe_modes, fwd, inv):
    modes, _, width, _ = probe_modes.shape
    vmem = pl.BlockSpec(memory_space=pltpu.VMEM)
    smem = pl.BlockSpec(memory_space=pltpu.SMEM)
    return pl.pallas_call(
        gradient_kernel,
        out_shape=jax.ShapeDtypeStruct(extended.shape, jnp.float32),
        in_specs=[smem, smem] + [vmem] * 5,
        out_specs=vmem,
        scratch_shapes=[
            pltpu.VMEM((2, width, width), jnp.float32),
            pltpu.VMEM((modes, 2, width, width), jnp.bfloat16),
            pltpu.VMEM((modes, 2, width, width), jnp.bfloat16),
            pltpu.VMEM((modes, 2, width, width), jnp.float32),
            pltpu.VMEM((modes, 2, width, width), jnp.bfloat16),
            pltpu.VMEM((modes, 2, width, width), jnp.bfloat16),
            pltpu.VMEM((2, width, width), jnp.float32),
        ],
        compiler_params=pltpu.CompilerParams(vmem_limit_bytes=40 * 1024 * 1024),
        name="gradient",
    )(counts, positions, extended, amp, probe_modes, fwd, inv)


def exact(values, product):
    total = None
    for _ in range(3):
        piece = values.astype(jnp.bfloat16)
        values = values - piece.astype(jnp.float32)
        part = product(piece)
        total = part if total is None else total + part
    return total


def sort_kernel(amp_ref, perm_ref, back_ref, out_ref):
    def one(s, carry):
        cols = exact(amp_ref[s], lambda piece: dot(piece, perm_ref[...]))
        out_ref[s] = exact(cols, lambda piece: dot(back_ref[...], piece))
        return carry

    lax.fori_loop(0, amp_ref.shape[0], one, 0)


def sort_amplitude(amp):
    width = amp.shape[-1]
    perm = np.zeros((width, width), np.float32)
    order = np.concatenate([np.arange(0, width, 2), np.arange(1, width, 2)])
    perm[order, np.arange(width)] = 1.0
    return pl.pallas_call(
        sort_kernel,
        out_shape=jax.ShapeDtypeStruct(amp.shape, jnp.float32),
        in_specs=[pl.BlockSpec(memory_space=pltpu.VMEM)] * 3,
        out_specs=pl.BlockSpec(memory_space=pltpu.VMEM),
        cost_estimate=pl.CostEstimate(
            flops=12 * width**3 * amp.shape[0],
            bytes_accessed=8 * amp.size,
            transcendentals=0,
        ),
        name="sort_amplitude",
    )(amp, jnp.asarray(perm).astype(jnp.bfloat16), jnp.asarray(perm.T).astype(jnp.bfloat16))


def body(object_field, probe_modes, positions, counts, amplitude):
    width = probe_modes.shape[-1]
    tile = object_field.shape[1]
    fwd, inv = tables(width)
    amp = sort_amplitude(amplitude[0, 0])
    field = object_field
    (extended,) = exchange(None, field, True)
    for sweep in range(ITERS):
        total = gradient(counts, positions, extended, amp, probe_modes, fwd, inv)
        if sweep < ITERS - 1:
            field, extended = exchange(total, field, True)
        else:
            (field,) = exchange(total, field, False)
    return field


def solution(mesh):
    placed = (
        P(None, "row", "col"),
        P(),
        P("row", "col", None, None),
        P("row", "col"),
        P("row", "col", None, None, None),
    )
    return jax.shard_map(
        body, mesh=mesh, in_specs=placed, out_specs=P(None, "row", "col"), check_vma=False
    )
```
